128 devices in a mesh: rep: 1, data: 16 (over z, y), expert: 8 (over x, core).
Axes of the slice: x: 4, y: 4, z: 4, core: 2. Of those that a mesh axis runs over, the one named last changes fastest.
Arguments:
- tok_in: bfloat16 [262144, 512], P(('rep', 'expert', 'data'))
- expert_idx: int32 [262144, 8], P(('rep', 'expert', 'data'))
- gate_wt: float32 [262144, 8], P(('rep', 'expert', 'data'))
- w_gate: bfloat16 [128, 512, 192], P('expert', 'data')
- w_up: bfloat16 [128, 512, 192], P('expert', 'data')
- w_down: bfloat16 [128, 192, 512], P('expert', None, 'data')
- grad_out: bfloat16 [262144, 512], P(('rep', 'expert', 'data'))
Outputs:
- output 1: bfloat16 [262144, 512], P(('rep', 'expert', 'data'))
- output 2: bfloat16 [262144, 512], P(('rep', 'expert', 'data'))
- output 3: float32 [128, 512, 192], P(('rep', 'expert'), 'data')
- output 4: float32 [128, 512, 192], P(('rep', 'expert'), 'data')
- output 5: float32 [128, 192, 512], P(('rep', 'expert'), None, 'data')
All inputs are finite; a program needn't handle non-finite values.
Results may differ from the reference program's by a relative error of at most 0.001.
Values are sent between devices in bfloat16 or wider.
A program may use at most 1 GiB of HBM per device.

```python
import jax
import jax.numpy as jnp
from jax import lax

TOKENS = 2048
HIDDEN = 512
FFN_DIM = 192
EXPERTS = 128
TOP_K = 8
EP_SIZE = 8
DP_SIZE = 16

GROUP_DEVS = EP_SIZE * DP_SIZE
PART_TOKENS = GROUP_DEVS * TOKENS
CAPACITY = (5 * TOP_K * TOKENS + 4 * EXPERTS - 1) // (4 * EXPERTS)
HOT_COUNT = max(1, EXPERTS // 8)
TOTAL_ROWS = EXPERTS * GROUP_DEVS * CAPACITY


def draw_routing(route_key, hot_key):
    expert_perm = jax.random.permutation(hot_key, EXPERTS)
    hot_bonus = jnp.where(expert_perm < HOT_COUNT, 6554, 0)
    local_tok = jnp.arange(PART_TOKENS) % TOKENS
    forced = (local_tok[:, None] < CAPACITY) & (expert_perm[None, :] == 0)
    scores = jax.random.randint(route_key, (PART_TOKENS, EXPERTS), 0, 65536, dtype=jnp.int32)
    scores = scores + hot_bonus[None, :] + jnp.where(forced, 131072, 0)
    keyed_scores = scores * EXPERTS + jnp.arange(EXPERTS, dtype=jnp.int32)[None, :]
    return lax.top_k(keyed_scores, TOP_K)[1].astype(jnp.int32)


def setup_inputs(seed: int = 0, part: int = 0) -> dict:
    shared_keys = jax.random.split(jax.random.key(seed), 3)
    part_keys = jax.random.split(jax.random.fold_in(jax.random.key(seed + 1), part), 5)
    tok_in = jax.random.normal(part_keys[0], (PART_TOKENS, HIDDEN), jnp.float32).astype(jnp.bfloat16)
    expert_idx = draw_routing(part_keys[1], part_keys[2])
    gate_wt = jax.random.uniform(part_keys[3], (PART_TOKENS, TOP_K), jnp.float32, 0.5, 1.5) * TOP_K ** -0.5
    w_gate = (jax.random.normal(shared_keys[0], (EXPERTS, HIDDEN, FFN_DIM), jnp.float32) * HIDDEN ** -0.5).astype(jnp.bfloat16)
    w_up = (jax.random.normal(shared_keys[1], (EXPERTS, HIDDEN, FFN_DIM), jnp.float32) * HIDDEN ** -0.5).astype(jnp.bfloat16)
    w_down = (jax.random.normal(shared_keys[2], (EXPERTS, FFN_DIM, HIDDEN), jnp.float32) * (1.6 * FFN_DIM ** -0.5)).astype(jnp.bfloat16)
    grad_out = jax.random.normal(part_keys[4], (PART_TOKENS, HIDDEN), jnp.float32).astype(jnp.bfloat16)
    return dict(tok_in=tok_in, expert_idx=expert_idx, gate_wt=gate_wt, w_gate=w_gate, w_up=w_up, w_down=w_down, grad_out=grad_out)


def expert_step(operands):
    exp_rows, exp_cots, gate_mat, up_mat, down_mat = operands
    pre_gate = jnp.dot(exp_rows, gate_mat, preferred_element_type=jnp.float32)
    pre_up = jnp.dot(exp_rows, up_mat, preferred_element_type=jnp.float32)
    sig_gate = jax.nn.sigmoid(pre_gate)
    silu_gate = pre_gate * sig_gate
    hid_act = (silu_gate * pre_up).astype(jnp.bfloat16)
    exp_out = jnp.dot(hid_act, down_mat, preferred_element_type=jnp.float32).astype(jnp.bfloat16)
    grad_down = jnp.dot(hid_act.T, exp_cots, preferred_element_type=jnp.float32)
    grad_hid = jnp.dot(exp_cots, down_mat.T, preferred_element_type=jnp.float32)
    grad_pre_gate = (grad_hid * pre_up * sig_gate * (1.0 + pre_gate * (1.0 - sig_gate))).astype(jnp.bfloat16)
    grad_pre_up = (grad_hid * silu_gate).astype(jnp.bfloat16)
    grad_gate = jnp.dot(exp_rows.T, grad_pre_gate, preferred_element_type=jnp.float32)
    grad_up = jnp.dot(exp_rows.T, grad_pre_up, preferred_element_type=jnp.float32)
    grad_rows = (jnp.dot(grad_pre_gate, gate_mat.T, preferred_element_type=jnp.float32) + jnp.dot(grad_pre_up, up_mat.T, preferred_element_type=jnp.float32)).astype(jnp.bfloat16)
    return exp_out, grad_rows, grad_gate, grad_up, grad_down


def reference(tok_in, expert_idx, gate_wt, w_gate, w_up, w_down, grad_out):
    pair_ids = expert_idx.reshape(GROUP_DEVS, TOKENS * TOP_K)
    expert_hits = (pair_ids[:, :, None] == jnp.arange(EXPERTS, dtype=jnp.int32)[None, None, :]).astype(jnp.int32)
    pair_slot = jnp.sum((jnp.cumsum(expert_hits, axis=1) - expert_hits) * expert_hits, axis=2)
    dev_ids = jnp.arange(GROUP_DEVS, dtype=jnp.int32)[:, None]
    flat_dest = jnp.where(pair_slot < CAPACITY, (pair_ids * GROUP_DEVS + dev_ids) * CAPACITY + pair_slot, TOTAL_ROWS).reshape(-1)
    tok_pairs = jnp.repeat(tok_in, TOP_K, axis=0)
    cot_pairs = (gate_wt.reshape(-1, 1) * jnp.repeat(grad_out, TOP_K, axis=0).astype(jnp.float32)).astype(jnp.bfloat16)
    row_buf = jnp.zeros((TOTAL_ROWS, HIDDEN), jnp.bfloat16).at[flat_dest].set(tok_pairs, mode="drop")
    cot_buf = jnp.zeros((TOTAL_ROWS, HIDDEN), jnp.bfloat16).at[flat_dest].set(cot_pairs, mode="drop")
    exp_out, grad_rows, grad_gate, grad_up, grad_down = lax.map(expert_step, (row_buf.reshape(EXPERTS, GROUP_DEVS * CAPACITY, HIDDEN), cot_buf.reshape(EXPERTS, GROUP_DEVS * CAPACITY, HIDDEN), w_gate, w_up, w_down))
    pair_out = jnp.take(exp_out.reshape(TOTAL_ROWS, HIDDEN), flat_dest, axis=0, mode="fill", fill_value=0).reshape(PART_TOKENS, TOP_K, HIDDEN)
    pair_grad = jnp.take(grad_rows.reshape(TOTAL_ROWS, HIDDEN), flat_dest, axis=0, mode="fill", fill_value=0).reshape(PART_TOKENS, TOP_K, HIDDEN)
    tok_out = (tok_in.astype(jnp.float32) + jnp.sum(gate_wt[:, :, None] * pair_out.astype(jnp.float32), axis=1)).astype(jnp.bfloat16)
    grad_in = (grad_out.astype(jnp.float32) + jnp.sum(pair_grad.astype(jnp.float32), axis=1)).astype(jnp.bfloat16)
    return tok_out, grad_in, grad_gate, grad_up, grad_down
```

```python
import functools

import jax
import jax.numpy as jnp
from jax import lax
from jax.experimental import pallas as pl
from jax.experimental.pallas import tpu as pltpu
from jax.sharding import PartitionSpec as P


LANES = 128
GROUP = 3072
VMEM_BIG = 60 * 1024 * 1024


def ceil_to(n, m):
    return (n + m - 1) // m * m


def call(body, interpret=False, **kw):
    return pl.pallas_call(body, **kw)


def route_body(cap, stride, n_loc, ids_ref, dest_ref):
    top_k, tokens = ids_ref.shape
    n_exp = 128
    blk = min(256, tokens)
    before = (lax.broadcasted_iota(jnp.int32, (blk, blk), 0) < lax.broadcasted_iota(jnp.int32, (blk, blk), 1)).astype(jnp.bfloat16)
    exp_iota = lax.broadcasted_iota(jnp.int32, (n_exp, blk), 0)
    n_pos = n_exp // n_loc
    base = jnp.zeros((n_exp, 1), jnp.float32)
    for b in range(tokens // blk):
        ids = ids_ref[:, b * blk : (b + 1) * blk]
        hits = [exp_iota == ids[j : j + 1, :] for j in range(top_k)]
        any_hit = functools.reduce(jnp.logical_or, hits)
        hot = jnp.where(any_hit, 1.0, 0.0)
        rank = jnp.dot(hot.astype(jnp.bfloat16), before, preferred_element_type=jnp.float32) + base
        base = base + jnp.sum(hot, axis=1, keepdims=True)
        rows = []
        for j in range(top_k):
            slot = jnp.sum(jnp.where(hits[j], rank, 0.0), axis=0, keepdims=True).astype(jnp.int32)
            e = ids[j : j + 1, :]
            rows.append(jnp.where(slot < cap, (e // n_loc) * GROUP + (e % n_loc) * stride + slot, n_pos * GROUP))
        dest_ref[:, b * blk : (b + 1) * blk] = jnp.concatenate(rows, axis=0)


def list_body(top_k, tokens, fill_ref, dest_ref, list_ref, sem):
    copy = pltpu.make_async_copy(fill_ref, list_ref, sem)
    copy.start()
    copy.wait()
    unroll = 4

    def step(i, carry):
        for u in range(unroll):
            t = i * unroll + u
            for j in range(top_k):
                list_ref[dest_ref[j * tokens + t]] = t * top_k + j
        return carry

    lax.fori_loop(0, tokens // unroll, step, 0)


def make_list(expert_idx, cap, stride, n_loc):
    tokens, top_k = expert_idx.shape
    n_pos = 128 // n_loc
    dest = pl.pallas_call(
        functools.partial(route_body, cap, stride, n_loc),
        out_shape=jax.ShapeDtypeStruct((top_k, tokens), jnp.int32),
        in_specs=[pl.BlockSpec(memory_space=pltpu.VMEM)],
        out_specs=pl.BlockSpec(memory_space=pltpu.VMEM),
        cost_estimate=pl.CostEstimate(flops=4_000_000_000, bytes_accessed=1 << 17, transcendentals=0),
        name="route",
    )(expert_idx.T)
    size = n_pos * GROUP + 1024
    fill = jnp.full((size,), tokens * top_k, jnp.int32)
    return pl.pallas_call(
        functools.partial(list_body, top_k, tokens),
        out_shape=jax.ShapeDtypeStruct((size,), jnp.int32),
        in_specs=[pl.BlockSpec(memory_space=pl.ANY), pl.BlockSpec(memory_space=pltpu.SMEM)],
        out_specs=pl.BlockSpec(memory_space=pltpu.SMEM),
        scratch_shapes=[pltpu.SemaphoreType.DMA],
        cost_estimate=pl.CostEstimate(flops=10_000_000_000, bytes_accessed=1 << 17, transcendentals=0),
        name="lists",
    )(fill, dest.reshape(-1))


def load_lists(groups_ref, list_ref, gate_ref, lists, gates, sems):
    copies = [pltpu.make_async_copy(list_ref.at[pl.ds(pl.multiple_of(groups_ref[g] * GROUP, GROUP), GROUP)], lists.at[pl.ds(g * GROUP, GROUP)], sems.at[g]) for g in range(2)]
    copies.append(pltpu.make_async_copy(gate_ref, gates, sems.at[2]))
    for c in copies:
        c.start()
    for c in copies:
        c.wait()


def dispatch_body(n_blk, stride, top_k, n_loc, groups_ref, list_ref, gate_ref, x_ref, dy_ref, r_ref, c_ref, lists, gates, rows, tile, sems):
    i = pl.program_id(0)
    tokens, width = x_ref.shape
    parts = width // LANES
    slab = 2 * parts
    span = stride + 1

    @pl.when(i == 0)
    def _():
        load_lists(groups_ref, list_ref, gate_ref, lists, gates, sems)
        rows[pl.ds(tokens * slab, slab), :] = jnp.zeros((slab, LANES), jnp.float32)

        def fill(b, carry):
            t0 = pl.multiple_of(b * 16, 16)
            xs = x_ref[pl.ds(t0, 16), :].astype(jnp.float32)
            ds = dy_ref[pl.ds(t0, 16), :].astype(jnp.float32)
            for k in range(parts):
                rows[pl.ds(t0 * slab + k, 16, stride=slab), :] = xs[:, k * LANES : (k + 1) * LANES]
                rows[pl.ds(t0 * slab + parts + k, 16, stride=slab), :] = ds[:, k * LANES : (k + 1) * LANES]
            return carry

        lax.fori_loop(0, tokens // 16, fill, 0)

    upper = lax.broadcasted_iota(jnp.int32, (slab, LANES), 0) < parts
    for b in range(n_blk):
        e = i * n_blk + b
        base = (e // n_loc) * GROUP + (e % n_loc) * stride

        def gather(q, carry, base=base):
            for u in range(16):
                s = q * 16 + u
                p = lists[base + s]
                row = rows[pl.ds(pl.multiple_of((p // top_k) * slab, slab), slab), :]
                tile[pl.ds(s, slab, stride=span), :] = row * jnp.where(upper, 1.0, gates[p])
            return carry

        lax.fori_loop(0, stride // 16, gather, 0)
        for k in range(parts):
            r_ref[b, :, k * LANES : (k + 1) * LANES] = tile[pl.ds(k * span, stride), :].astype(jnp.bfloat16)
            c_ref[b, :, k * LANES : (k + 1) * LANES] = tile[pl.ds((parts + k) * span, stride), :].astype(jnp.bfloat16)


def dispatch(groups, lists, gates, x, dy, stride, top_k, n_loc, n_blk=4):
    tokens, width = x.shape
    slab = 2 * (width // LANES)
    n_mine = 2 * n_loc
    shape = jax.ShapeDtypeStruct((n_mine, stride, width), jnp.bfloat16)
    spec = pl.BlockSpec((n_blk, stride, width), lambda i: (i, 0, 0))
    return pl.pallas_call(
        functools.partial(dispatch_body, n_blk, stride, top_k, n_loc),
        grid=(n_mine // n_blk,),
        out_shape=(shape, shape),
        in_specs=[
            pl.BlockSpec(memory_space=pltpu.SMEM),
            pl.BlockSpec(memory_space=pl.ANY),
            pl.BlockSpec(memory_space=pl.ANY),
            pl.BlockSpec(memory_space=pltpu.VMEM),
            pl.BlockSpec(memory_space=pltpu.VMEM),
        ],
        out_specs=(spec, spec),
        scratch_shapes=[
            pltpu.SMEM((2 * GROUP,), jnp.int32),
            pltpu.SMEM(gates.shape, jnp.float32),
            pltpu.VMEM(((tokens + 1) * slab, LANES), jnp.float32),
            pltpu.VMEM((ceil_to(slab * (stride + 1), 8), LANES), jnp.float32),
            pltpu.SemaphoreType.DMA((3,)),
        ],
        compiler_params=pltpu.CompilerParams(dimension_semantics=("arbitrary",), vmem_limit_bytes=VMEM_BIG),
        cost_estimate=pl.CostEstimate(flops=10_000_000_000, bytes_accessed=1 << 24, transcendentals=0),
        name="dispatch",
    )(groups, lists, gates, x, dy)


def combine_body(n_blk, stride, top_k, n_loc, groups_ref, list_ref, gate_ref, o_ref, dr_ref, out_ref, lists, gates, acc, tile, sems):
    i = pl.program_id(0)
    tokens = out_ref.shape[0]
    width = o_ref.shape[-1]
    parts = width // LANES
    slab = 2 * parts
    span = stride + 1

    @pl.when(i == 0)
    def _():
        load_lists(groups_ref, list_ref, gate_ref, lists, gates, sems)

        def clear(b, carry):
            acc[pl.ds(pl.multiple_of(b * 8 * slab, 8 * slab), 8 * slab), :] = jnp.zeros((8 * slab, LANES), jnp.float32)
            return carry

        lax.fori_loop(0, tokens // 8, clear, 0)

    upper = lax.broadcasted_iota(jnp.int32, (slab, LANES), 0) < parts
    for b in range(n_blk):
        e = i * n_blk + b
        base = (e // n_loc) * GROUP + (e % n_loc) * stride
        for k in range(parts):
            tile[pl.ds(k * span, stride), :] = o_ref[0, b, :, k * LANES : (k + 1) * LANES].astype(jnp.float32)
            tile[pl.ds((parts + k) * span, stride), :] = dr_ref[0, b, :, k * LANES : (k + 1) * LANES].astype(jnp.float32)

        def scatter(q, carry, base=base):
            for half in range(2):
                at, sums = [], []
                for u in range(8):
                    s = q * 16 + half * 8 + u
                    p = lists[base + s]
                    a = pl.multiple_of((p // top_k) * slab, slab)
                    row = tile[pl.ds(s, slab, stride=span), :] * jnp.where(upper, gates[p], 1.0)
                    at.append(a)
                    sums.append(acc[pl.ds(a, slab), :] + row)
                for a, v in zip(at, sums):
                    acc[pl.ds(a, slab), :] = v
            return carry

        lax.fori_loop(0, stride // 16, scatter, 0)

    @pl.when(i == pl.num_programs(0) - 1)
    def _():
        def write(b, carry):
            t0 = pl.multiple_of(b * 8, 8)
            for k in range(slab):
                out_ref[pl.ds(t0, 8), k * LANES : (k + 1) * LANES] = acc[pl.ds(t0 * slab + k, 8, stride=slab), :]
            return carry

        lax.fori_loop(0, tokens // 8, write, 0)


def combine(block, groups, lists, gates, o, dr, tokens, stride, top_k, n_loc, n_blk=4):
    width = o.shape[-1]
    slab = 2 * (width // LANES)
    n_mine = 2 * n_loc
    spec = pl.BlockSpec((1, n_blk, stride, width), lambda i: (block, i, 0, 0))
    return pl.pallas_call(
        functools.partial(combine_body, n_blk, stride, top_k, n_loc),
        grid=(n_mine // n_blk,),
        out_shape=jax.ShapeDtypeStruct((tokens, 2 * width), jnp.float32),
        in_specs=[
            pl.BlockSpec(memory_space=pltpu.SMEM),
            pl.BlockSpec(memory_space=pl.ANY),
            pl.BlockSpec(memory_space=pl.ANY),
            spec,
            spec,
        ],
        out_specs=pl.BlockSpec(memory_space=pltpu.VMEM),
        scratch_shapes=[
            pltpu.SMEM((2 * GROUP,), jnp.int32),
            pltpu.SMEM(gates.shape, jnp.float32),
            pltpu.VMEM(((tokens + 1) * slab, LANES), jnp.float32),
            pltpu.VMEM((ceil_to(slab * (stride + 1), 8), LANES), jnp.float32),
            pltpu.SemaphoreType.DMA((3,)),
        ],
        compiler_params=pltpu.CompilerParams(dimension_semantics=("arbitrary",), vmem_limit_bytes=VMEM_BIG),
        cost_estimate=pl.CostEstimate(flops=14_000_000_000, bytes_accessed=1 << 24, transcendentals=0),
        name="combine",
    )(groups, lists, gates, o, dr)


def pack_body(g_ref, u_ref, d_ref, out_ref):
    n, rows, _ = g_ref.shape
    half = rows // 2
    low = lax.broadcasted_iota(jnp.int32, (half, LANES), 1) < LANES // 2
    for e in range(n):
        for m, ref in enumerate((g_ref, u_ref, d_ref)):
            base = m * (rows + half)
            out_ref[e, base : base + rows, :] = ref[e, :, :LANES]
            rest = jnp.concatenate([ref[e, :, LANES:], jnp.zeros((rows, LANES // 2), ref.dtype)], axis=1).astype(jnp.float32)
            both = jnp.where(low, rest[:half], pltpu.roll(rest[half:], LANES // 2, 1))
            out_ref[e, base + rows : base + rows + half, :] = both.astype(out_ref.dtype)


def pack_weights(w_gate, w_up, w_down_t):
    n, rows, _ = w_gate.shape
    return pl.pallas_call(
        pack_body,
        out_shape=jax.ShapeDtypeStruct((n, 3 * (rows + rows // 2), LANES), w_gate.dtype),
        cost_estimate=pl.CostEstimate(flops=1_000_000_000, bytes_accessed=1 << 21, transcendentals=0),
        name="pack",
    )(w_gate, w_up, w_down_t)


def unpack_body(half_n, n_in, *refs):
    ins, outs = refs[: 2 * n_in], refs[2 * n_in :]
    rows = outs[0].shape[1]
    half = rows // 2
    at = 0
    for k in range(n_in):
        mine, theirs = ins[2 * k], ins[2 * k + 1]
        for e in range(half_n):
            for m, out in enumerate(outs):
                base = m * (rows + half)
                out[at, :, :LANES] = mine[e, base : base + rows, :] + theirs[e, base : base + rows, :]
                rest = mine[e, base + rows : base + rows + half, :] + theirs[e, base + rows : base + rows + half, :]
                out[at, :half, LANES:] = rest[:, : LANES // 2]
                out[at, half:, LANES:] = pltpu.roll(rest, LANES // 2, 1)[:, : LANES // 2]
            at += 1


def unpack_grads(pairs, n_loc, rows, f_dim):
    half_n = pairs[0][1].shape[0]
    shape = jax.ShapeDtypeStruct((n_loc, rows, f_dim), jnp.float32)
    flat = [a for p in pairs for a in p]
    return pl.pallas_call(
        functools.partial(unpack_body, half_n, len(pairs)),
        out_shape=(shape,) * 3,
        cost_estimate=pl.CostEstimate(flops=1_000_000_000, bytes_accessed=1 << 22, transcendentals=0),
        compiler_params=pltpu.CompilerParams(vmem_limit_bytes=VMEM_BIG),
        name="unpack",
    )(*flat)


def shard_index(z, y, first, a, b, sign):
    dz, dy = (a, b) if first == "z" else (b, a)
    return lax.rem(z + sign * dz + 4, 4) * 4 + lax.rem(y + sign * dy + 4, 4)


def experts_body(n_sets, last, first, has_prev, *refs):
    place = refs[0]
    r_refs = refs[1 : 1 + n_sets]
    c_refs = refs[1 + n_sets : 1 + 2 * n_sets]
    at = 1 + 2 * n_sets
    w_refs = refs[at : at + 5]
    at += 5 + (2 if has_prev else 0)
    o_ref, dr_ref = refs[at : at + 2]
    g_refs = refs[at + 2 : at + 7]
    wgu, wd, ab, dh, hid, dab, dwgu, dwd = refs[at + 7 :]
    z, y = place[0], place[1]
    stride, width = r_refs[0].shape[1:]
    rows = width // 16
    half = rows // 2
    packed = rows + half
    f_pad = wd.shape[1]
    low = lax.broadcasted_iota(jnp.int32, (half, LANES), 1) < LANES // 2

    for a in range(4):
        for b in range(4):
            if a == 2:
                ref, slot = (w_refs[3], b) if b < 2 else (w_refs[4], b - 2)
            else:
                ref, slot = w_refs[(0, 1, None, 2)[a]], b
            k = shard_index(z, y, last, a, b, -1)
            row0 = pl.multiple_of(k * rows, rows)
            for m in range(3):
                base = m * packed
                dst, col = (wgu, m * f_pad) if m < 2 else (wd, 0)
                dst[pl.ds(row0, rows), col : col + LANES] = ref[slot, 0, base : base + rows, :]
                rest = ref[slot, 0, base + rows : base + packed, :].astype(jnp.float32)
                top = jnp.where(low, rest, 0.0)
                bottom = jnp.where(low, pltpu.roll(rest, LANES // 2, 1), 0.0)
                dst[pl.ds(row0, rows), col + LANES : col + 2 * LANES] = jnp.concatenate([top, bottom], axis=0).astype(dst.dtype)

    rows_all = jnp.concatenate([r[0] for r in r_refs], axis=0)
    cots_all = jnp.concatenate([c[0] for c in c_refs], axis=0)
    ab[...] = jnp.dot(rows_all, wgu[...], preferred_element_type=jnp.float32)
    dh[...] = jnp.dot(cots_all, wd[...], preferred_element_type=jnp.float32)

    def act(q, carry):
        r0 = pl.multiple_of(q * 32, 32)
        pre = ab[pl.ds(r0, 32), :f_pad]
        up = ab[pl.ds(r0, 32), f_pad:]
        grad = dh[pl.ds(r0, 32), :]
        sig = jax.nn.sigmoid(pre)
        silu = pre * sig
        hid[pl.ds(r0, 32), :] = (silu * up).astype(jnp.bfloat16)
        dab[pl.ds(r0, 32), :f_pad] = (grad * up * sig * (1.0 + pre * (1.0 - sig))).astype(jnp.bfloat16)
        dab[pl.ds(r0, 32), f_pad:] = (grad * silu).astype(jnp.bfloat16)
        return carry

    lax.fori_loop(0, n_sets * stride // 32, act, 0)

    nt = (((1,), (1,)), ((), ()))
    tn = (((0,), (0,)), ((), ()))
    out = lax.dot_general(hid[...], wd[...], nt, preferred_element_type=jnp.float32).astype(jnp.bfloat16)
    for s in range(n_sets):
        o_ref[s, 0] = out[s * stride : (s + 1) * stride]
    back = lax.dot_general(dab[...], wgu[...], nt, preferred_element_type=jnp.float32).astype(jnp.bfloat16)
    for s in range(n_sets):
        dr_ref[s, 0] = back[s * stride : (s + 1) * stride]
    dwgu[...] = lax.dot_general(rows_all, dab[...], tn, preferred_element_type=jnp.float32)
    dwd[...] = lax.dot_general(cots_all, hid[...], tn, preferred_element_type=jnp.float32)

    for a in range(4):
        for b in range(4):
            if a == 2:
                ref, slot = (g_refs[3], b) if b < 2 else (g_refs[4], b - 2)
            else:
                ref, slot = g_refs[(0, 1, None, 2)[a]], b
            k = shard_index(z, y, first, a, b, 1)
            row0 = pl.multiple_of(k * rows, rows)
            for m in range(3):
                base = m * packed
                src, col = (dwgu, m * f_pad) if m < 2 else (dwd, 0)
                ref[slot, 0, base : base + rows, :] = src[pl.ds(row0, rows), col : col + LANES]
                rest = src[pl.ds(row0, rows), col + LANES : col + 2 * LANES]
                ref[slot, 0, base + rows : base + packed, :] = jnp.where(low, rest[:half], pltpu.roll(rest[half:], LANES // 2, 1))


def experts(place, r_sets, c_sets, w_arrays, prev, colour, start, count, n_loc):
    n_sets = len(r_sets)
    n_mine, stride, width = r_sets[0].shape
    half_n = n_loc // 2
    packed = w_arrays[0].shape[2]
    off = colour * half_n + start
    first, last = ("y", "z") if colour == 0 else ("z", "y")
    total = 2 * count

    def mine(i):
        return jnp.where(i < count, off + i, n_loc + off + i - count)

    def held(i):
        return jnp.where(i < count, start + i, half_n + start + i - count)

    tok_spec = pl.BlockSpec((1, stride, width), lambda i: (mine(i), 0, 0))
    out_spec = pl.BlockSpec((n_sets, 1, stride, width), lambda i: (0, mine(i), 0, 0))
    out_shape = jax.ShapeDtypeStruct((n_sets, n_mine, stride, width), jnp.bfloat16)
    f_pad = 2 * LANES
    m_rows = n_sets * stride
    w_specs = [pl.BlockSpec((w.shape[0], 1, packed, LANES), lambda i: (0, held(i), 0, 0)) for w in w_arrays]
    g_slots = (4, 4, 4, 2, 2)
    g_specs = [pl.BlockSpec((n, 1, packed, LANES), lambda i: (0, i, 0, 0)) for n in g_slots]
    g_shapes = [jax.ShapeDtypeStruct((n, total, packed, LANES), jnp.float32) for n in g_slots]
    in_specs = [pl.BlockSpec(memory_space=pltpu.SMEM)] + [tok_spec] * (2 * n_sets) + w_specs
    args = [place, *r_sets, *c_sets, *w_arrays]
    aliases = {}
    if prev is not None:
        aliases = {len(args): 0, len(args) + 1: 1}
        in_specs += [pl.BlockSpec(memory_space=pl.ANY)] * 2
        args += list(prev)
    res = pl.pallas_call(
        functools.partial(experts_body, n_sets, last, first, prev is not None),
        grid=(total,),
        out_shape=[out_shape, out_shape] + g_shapes,
        in_specs=in_specs,
        out_specs=[out_spec, out_spec] + g_specs,
        scratch_shapes=[
            pltpu.VMEM((width, 2 * f_pad), jnp.bfloat16),
            pltpu.VMEM((width, f_pad), jnp.bfloat16),
            pltpu.VMEM((m_rows, 2 * f_pad), jnp.float32),
            pltpu.VMEM((m_rows, f_pad), jnp.float32),
            pltpu.VMEM((m_rows, f_pad), jnp.bfloat16),
            pltpu.VMEM((m_rows, 2 * f_pad), jnp.bfloat16),
            pltpu.VMEM((width, 2 * f_pad), jnp.float32),
            pltpu.VMEM((width, f_pad), jnp.float32),
        ],
        input_output_aliases=aliases,
        compiler_params=pltpu.CompilerParams(dimension_semantics=("arbitrary",), vmem_limit_bytes=VMEM_BIG),
        cost_estimate=pl.CostEstimate(flops=3_000_000_000 * total, bytes_accessed=6_000_000 * total, transcendentals=0),
        name="experts",
    )(*args)
    return (res[0], res[1]), res[2:]


def solution(mesh):
    n_pos = mesh.shape["expert"]
    chips_x = n_pos // 2
    row_spec = P(("rep", "expert", "data"), None)
    wide_spec = P("expert", "data", None)
    down_spec = P("expert", None, "data")
    wide_out = P(("rep", "expert"), "data", None)
    down_out = P(("rep", "expert"), None, "data")

    def y_perm(d):
        return [(z * 4 + y, z * 4 + (y + d) % 4) for z in range(4) for y in range(4)]

    def z_perm(d):
        return [(z * 4 + y, (z + d) % 4 * 4 + y) for z in range(4) for y in range(4)]

    perms = {"y": y_perm, "z": z_perm}
    partner = [(p, (p + n_pos // 2) % n_pos) for p in range(n_pos)]
    mate = [(p, p ^ 1) for p in range(n_pos)]
    to_neighbour = [(p, (p + (2 if p % 2 == 0 else -2)) % n_pos) for p in range(n_pos)]
    to_home = [(b, a) for a, b in to_neighbour]

    def step_along(v, axis, d):
        return lax.ppermute(v, "data", perms[axis](d))

    def gather_ring(v, axis, cut):
        one = step_along(v, axis, 1)
        three = step_along(v, axis, 3)
        two_a = step_along(one[:cut], axis, 1)
        two_b = step_along(three[cut:], axis, 3)
        return v, one, three, two_a, two_b

    def scatter_ring(parts, axis, cut):
        zero, one, three, two_a, two_b = parts
        in_a = step_along(two_a, axis, 1)
        in_b = step_along(two_b, axis, 3)
        one = one.at[:cut].add(in_a)
        three = three.at[cut:].add(in_b)
        return zero, step_along(one, axis, 1), step_along(three, axis, 3)

    def local_step(tok_in, expert_idx, gate_wt, w_gate, w_up, w_down, grad_out):
        tokens, top_k = expert_idx.shape
        width = tok_in.shape[1]
        n_loc, rows, f_dim = w_gate.shape
        n_exp = n_loc * n_pos
        cap = (5 * top_k * tokens + 4 * n_exp - 1) // (4 * n_exp)
        stride = ceil_to(cap, 16)
        half_n = n_loc // 2
        data_id = lax.axis_index("data")
        pos_id = lax.axis_index("expert")
        place = jnp.stack([data_id // 4, data_id % 4]).astype(jnp.int32)
        groups = jnp.stack([pos_id, (pos_id + n_pos // 2) % n_pos]).astype(jnp.int32)

        own = pack_weights(w_gate, w_up, jnp.swapaxes(w_down, 1, 2))
        other = lax.ppermute(own, "expert", partner)
        held = []
        for colour, (first, last) in enumerate((("y", "z"), ("z", "y"))):
            part = slice(colour * half_n, (colour + 1) * half_n)
            v = jnp.concatenate([own[part], other[part]], axis=0)
            v, one, three, two_a, two_b = gather_ring(v, first, half_n)
            four = jnp.stack([v, one, jnp.concatenate([two_a, two_b], axis=0), three])
            held.append(gather_ring(four, last, 2))

        gates = jnp.concatenate([gate_wt.reshape(-1), jnp.zeros((1024,), jnp.float32)])
        lists = make_list(expert_idx, cap, stride, n_loc)
        sets = [(tok_in, grad_out, gates, lists)]
        sets.append(tuple(lax.ppermute(a, "expert", mate) for a in sets[0]))
        sets.append(tuple(lax.ppermute(a, "expert", to_neighbour) for a in sets[0]))
        sets.append(tuple(lax.ppermute(a, "expert", mate) for a in sets[2]))
        sent = [dispatch(groups, li, g, x, d, stride, top_k, n_loc) for x, d, g, li in sets]
        r_sets, c_sets = [s[0] for s in sent], [s[1] for s in sent]

        prev = None
        grads = {}
        n_chunks = 2
        count = half_n // n_chunks
        for chunk in range(n_chunks):
            for colour in range(2):
                prev, parts = experts(place, r_sets, c_sets, held[colour], prev, colour, chunk * count, count, n_loc)
                first, last = ("y", "z") if colour == 0 else ("z", "y")
                zero, one, three = scatter_ring((parts[0], parts[1], parts[2], parts[3], parts[4]), first, 2)
                s = [zero[q] + one[q] + three[q] for q in range(4)]
                zero, one, three = scatter_ring((s[0], s[1], s[3], s[2][:count], s[2][count:]), last, count)
                mine = zero[:count] + one[:count] + three[:count]
                theirs = zero[count:] + one[count:] + three[count:]
                grads[colour, chunk] = (mine, lax.ppermute(theirs, "expert", partner))
        o_all, dr_all = prev

        sums = [combine(k, groups, sets[k][3], sets[k][2], o_all, dr_all, tokens, stride, top_k, n_loc) for k in (3, 2, 1, 0)][::-1]
        near = sums[2] + lax.ppermute(sums[3], "expert", mate)
        far = lax.ppermute(near, "expert", to_home)
        total = sums[0] + lax.ppermute(sums[1], "expert", mate) + far
        tok_out = (tok_in.astype(jnp.float32) + total[:, :width]).astype(jnp.bfloat16)
        grad_in = (grad_out.astype(jnp.float32) + total[:, width:]).astype(jnp.bfloat16)

        order = [grads[colour, chunk] for colour in range(2) for chunk in range(n_chunks)]
        gg, gu, gd = unpack_grads(order, n_loc, rows, f_dim)
        return tok_out, grad_in, gg, gu, jnp.swapaxes(gd, 1, 2)

    return jax.shard_map(local_step, mesh=mesh, in_specs=(row_spec, row_spec, row_spec, wide_spec, wide_spec, down_spec, row_spec), out_specs=(row_spec, row_spec, wide_out, wide_out, down_out), check_vma=False)
```

```python
import functools

import jax
import jax.numpy as jnp
from jax import lax
from jax.experimental import pallas as pl
from jax.experimental.pallas import tpu as pltpu
from jax.sharding import PartitionSpec as P


LANES = 128
TAIL = 1024
VMEM_BIG = 60 * 1024 * 1024


def ceil_to(n, m):
    return (n + m - 1) // m * m


def starts_body(ids_ref, out_ref):
    top_k, tokens = ids_ref.shape
    blk = min(256, tokens)
    exp_iota = lax.broadcasted_iota(jnp.int32, (LANES, blk), 0)
    ones = jnp.ones((8, blk), jnp.bfloat16)
    total = jnp.zeros((8, LANES), jnp.float32)
    for b in range(tokens // blk):
        ids = ids_ref[:, b * blk : (b + 1) * blk]
        below = jnp.zeros((LANES, blk), jnp.float32)
        for j in range(top_k):
            below = below + jnp.where(ids[j : j + 1, :] < exp_iota, 1.0, 0.0)
        total = total + lax.dot_general(ones, below.astype(jnp.bfloat16), (((1,), (1,)), ((), ())), preferred_element_type=jnp.float32)
    out_ref[...] = total.astype(jnp.int32)


def make_lists(expert_idx, gate_wt):
    tokens, top_k = expert_idx.shape
    pairs = tokens * top_k
    starts = pl.pallas_call(
        starts_body,
        out_shape=jax.ShapeDtypeStruct((8, LANES), jnp.int32),
        cost_estimate=pl.CostEstimate(flops=2_000_000_000, bytes_accessed=1 << 17, transcendentals=0),
        name="starts",
    )(expert_idx.T)
    key = expert_idx.reshape(-1) * pairs + jnp.arange(pairs, dtype=jnp.int32)
    key, gates = lax.sort((key, gate_wt.reshape(-1)), num_keys=1, is_stable=False)
    rows = lax.rem(key, pairs) // top_k
    tail = jnp.full((TAIL - LANES,), pairs, jnp.int32)
    return jnp.concatenate([rows, starts[0], tail]), jnp.concatenate([gates, jnp.zeros((TAIL,), jnp.float32)])


def load_lists(list_ref, gate_ref, lists, gates, sems):
    copies = [pltpu.make_async_copy(list_ref, lists, sems.at[0]), pltpu.make_async_copy(gate_ref, gates, sems.at[1])]
    for c in copies:
        c.start()
    for c in copies:
        c.wait()


def expert_span(groups_ref, lists, pairs, cap, n_loc, i):
    e = groups_ref[i // n_loc] * n_loc + lax.rem(i, n_loc)
    start = lists[pairs + e]
    return start, jnp.minimum(lists[pairs + e + 1] - start, cap)


def dispatch_body(n_blk, stride, cap, n_loc, pairs, groups_ref, list_ref, gate_ref, x_ref, dy_ref, r_ref, c_ref, lists, gates, rows, tile, sems):
    i = pl.program_id(0)
    tokens, width = x_ref.shape
    parts = width // LANES
    slab = 2 * parts
    span = stride + 1

    @pl.when(i == 0)
    def _():
        load_lists(list_ref, gate_ref, lists, gates, sems)
        rows[pl.ds(tokens * slab, slab), :] = jnp.zeros((slab, LANES), jnp.float32)
        tile[...] = jnp.zeros_like(tile)

        def fill(b, carry):
            t0 = pl.multiple_of(b * 16, 16)
            xs = x_ref[pl.ds(t0, 16), :].astype(jnp.float32)
            ds = dy_ref[pl.ds(t0, 16), :].astype(jnp.float32)
            for k in range(parts):
                rows[pl.ds(t0 * slab + k, 16, stride=slab), :] = xs[:, k * LANES : (k + 1) * LANES]
                rows[pl.ds(t0 * slab + parts + k, 16, stride=slab), :] = ds[:, k * LANES : (k + 1) * LANES]
            return carry

        lax.fori_loop(0, tokens // 16, fill, 0)

    upper = lax.broadcasted_iota(jnp.int32, (slab, LANES), 0) < parts
    slots = lax.broadcasted_iota(jnp.int32, (stride, LANES), 0)
    for b in range(n_blk):
        start, count = expert_span(groups_ref, lists, pairs, cap, n_loc, i * n_blk + b)

        def gather(q, carry, start=start):
            s0 = q * 16
            at = start + s0
            for u in range(16):
                row = rows[pl.ds(pl.multiple_of(lists[at + u] * slab, slab), slab), :]
                tile[pl.ds(s0 + u, slab, stride=span), :] = row * jnp.where(upper, 1.0, gates[at + u])
            return carry

        lax.fori_loop(0, lax.shift_right_logical(count + 15, 4), gather, 0)
        keep = slots < count
        for k in range(parts):
            r_ref[b, :, k * LANES : (k + 1) * LANES] = jnp.where(keep, tile[pl.ds(k * span, stride), :], 0.0).astype(jnp.bfloat16)
            c_ref[b, :, k * LANES : (k + 1) * LANES] = jnp.where(keep, tile[pl.ds((parts + k) * span, stride), :], 0.0).astype(jnp.bfloat16)


def dispatch(groups, lists, gates, x, dy, stride, cap, n_loc, n_blk=4):
    tokens, width = x.shape
    slab = 2 * (width // LANES)
    n_mine = 2 * n_loc
    shape = jax.ShapeDtypeStruct((n_mine, stride, width), jnp.bfloat16)
    spec = pl.BlockSpec((n_blk, stride, width), lambda i: (i, 0, 0))
    return pl.pallas_call(
        functools.partial(dispatch_body, n_blk, stride, cap, n_loc, lists.shape[0] - TAIL),
        grid=(n_mine // n_blk,),
        out_shape=(shape, shape),
        in_specs=[
            pl.BlockSpec(memory_space=pltpu.SMEM),
            pl.BlockSpec(memory_space=pl.ANY),
            pl.BlockSpec(memory_space=pl.ANY),
            pl.BlockSpec(memory_space=pltpu.VMEM),
            pl.BlockSpec(memory_space=pltpu.VMEM),
        ],
        out_specs=(spec, spec),
        scratch_shapes=[
            pltpu.SMEM(lists.shape, jnp.int32),
            pltpu.SMEM(gates.shape, jnp.float32),
            pltpu.VMEM(((tokens + 1) * slab, LANES), jnp.float32),
            pltpu.VMEM((ceil_to(slab * (stride + 1), 8), LANES), jnp.float32),
            pltpu.SemaphoreType.DMA((2,)),
        ],
        compiler_params=pltpu.CompilerParams(dimension_semantics=("arbitrary",), vmem_limit_bytes=VMEM_BIG),
        cost_estimate=pl.CostEstimate(flops=10_000_000_000, bytes_accessed=1 << 24, transcendentals=0),
        name="dispatch",
    )(groups, lists, gates, x, dy)


def combine_body(n_blk, stride, cap, n_loc, pairs, groups_ref, list_ref, gate_ref, o_ref, dr_ref, out_ref, lists, gates, acc, tile, sems):
    i = pl.program_id(0)
    tokens = out_ref.shape[0]
    width = o_ref.shape[-1]
    parts = width // LANES
    slab = 2 * parts
    span = stride + 1

    @pl.when(i == 0)
    def _():
        load_lists(list_ref, gate_ref, lists, gates, sems)

        def clear(b, carry):
            acc[pl.ds(pl.multiple_of(b * 8 * slab, 8 * slab), 8 * slab), :] = jnp.zeros((8 * slab, LANES), jnp.float32)
            return carry

        lax.fori_loop(0, tokens // 8, clear, 0)

    upper = lax.broadcasted_iota(jnp.int32, (slab, LANES), 0) < parts
    for b in range(n_blk):
        start, count = expert_span(groups_ref, lists, pairs, cap, n_loc, i * n_blk + b)
        for k in range(parts):
            tile[pl.ds(k * span, stride), :] = o_ref[0, b, :, k * LANES : (k + 1) * LANES].astype(jnp.float32)
            tile[pl.ds((parts + k) * span, stride), :] = dr_ref[0, b, :, k * LANES : (k + 1) * LANES].astype(jnp.float32)

        def scatter(n, limit, s0, start):
            ats, sums = [], []
            for u in range(n):
                at = start + s0 + u
                t = lists[at] if limit is None else jnp.where(s0 + u < limit, lists[at], tokens)
                a = pl.multiple_of(t * slab, slab)
                row = tile[pl.ds(s0 + u, slab, stride=span), :] * jnp.where(upper, gates[at], 1.0)
                ats.append(a)
                sums.append(acc[pl.ds(a, slab), :] + row)
            for a, v in zip(ats, sums):
                acc[pl.ds(a, slab), :] = v

        def full(q, carry, start=start):
            scatter(8, None, q * 8, start)
            return carry

        whole = lax.shift_right_logical(count, 3)
        lax.fori_loop(0, whole, full, 0)

        @pl.when(whole * 8 < count)
        def _(start=start, count=count, whole=whole):
            scatter(8, count, whole * 8, start)

    @pl.when(i == pl.num_programs(0) - 1)
    def _():
        def write(b, carry):
            t0 = pl.multiple_of(b * 8, 8)
            for k in range(slab):
                out_ref[pl.ds(t0, 8), k * LANES : (k + 1) * LANES] = acc[pl.ds(t0 * slab + k, 8, stride=slab), :]
            return carry

        lax.fori_loop(0, tokens // 8, write, 0)


def combine(block, groups, lists, gates, o, dr, tokens, cap, n_loc, n_blk=4):
    stride, width = o.shape[2:]
    slab = 2 * (width // LANES)
    n_mine = 2 * n_loc
    spec = pl.BlockSpec((1, n_blk, stride, width), lambda i: (block, i, 0, 0))
    return pl.pallas_call(
        functools.partial(combine_body, n_blk, stride, cap, n_loc, lists.shape[0] - TAIL),
        grid=(n_mine // n_blk,),
        out_shape=jax.ShapeDtypeStruct((tokens, 2 * width), jnp.float32),
        in_specs=[
            pl.BlockSpec(memory_space=pltpu.SMEM),
            pl.BlockSpec(memory_space=pl.ANY),
            pl.BlockSpec(memory_space=pl.ANY),
            spec,
            spec,
        ],
        out_specs=pl.BlockSpec(memory_space=pltpu.VMEM),
        scratch_shapes=[
            pltpu.SMEM(lists.shape, jnp.int32),
            pltpu.SMEM(gates.shape, jnp.float32),
            pltpu.VMEM(((tokens + 1) * slab, LANES), jnp.float32),
            pltpu.VMEM((ceil_to(slab * (stride + 1), 8), LANES), jnp.float32),
            pltpu.SemaphoreType.DMA((2,)),
        ],
        compiler_params=pltpu.CompilerParams(dimension_semantics=("arbitrary",), vmem_limit_bytes=VMEM_BIG),
        cost_estimate=pl.CostEstimate(flops=14_000_000_000, bytes_accessed=1 << 24, transcendentals=0),
        name="combine",
    )(groups, lists, gates, o, dr)


def pack_body(g_ref, u_ref, d_ref, out_ref):
    n, rows, _ = g_ref.shape
    half = rows // 2
    low = lax.broadcasted_iota(jnp.int32, (half, LANES), 1) < LANES // 2
    for e in range(n):
        for m, ref in enumerate((g_ref, u_ref, d_ref)):
            base = m * (rows + half)
            out_ref[e, base : base + rows, :] = ref[e, :, :LANES]
            rest = jnp.concatenate([ref[e, :, LANES:], jnp.zeros((rows, LANES // 2), ref.dtype)], axis=1).astype(jnp.float32)
            both = jnp.where(low, rest[:half], pltpu.roll(rest[half:], LANES // 2, 1))
            out_ref[e, base + rows : base + rows + half, :] = both.astype(out_ref.dtype)


def pack_weights(w_gate, w_up, w_down_t):
    n, rows, _ = w_gate.shape
    return pl.pallas_call(
        pack_body,
        out_shape=jax.ShapeDtypeStruct((n, 3 * (rows + rows // 2), LANES), w_gate.dtype),
        cost_estimate=pl.CostEstimate(flops=1_000_000_000, bytes_accessed=1 << 21, transcendentals=0),
        name="pack",
    )(w_gate, w_up, w_down_t)


def unpack_body(half_n, n_in, *refs):
    ins, outs = refs[: 2 * n_in], refs[2 * n_in :]
    rows = outs[0].shape[1]
    half = rows // 2
    at = 0
    for k in range(n_in):
        mine, theirs = ins[2 * k], ins[2 * k + 1]
        for e in range(half_n):
            for m, out in enumerate(outs):
                base = m * (rows + half)
                out[at, :, :LANES] = mine[e, base : base + rows, :] + theirs[e, base : base + rows, :]
                rest = mine[e, base + rows : base + rows + half, :] + theirs[e, base + rows : base + rows + half, :]
                out[at, :half, LANES:] = rest[:, : LANES // 2]
                out[at, half:, LANES:] = pltpu.roll(rest, LANES // 2, 1)[:, : LANES // 2]
            at += 1


def unpack_grads(pairs, n_loc, rows, f_dim):
    half_n = pairs[0][1].shape[0]
    shape = jax.ShapeDtypeStruct((n_loc, rows, f_dim), jnp.float32)
    flat = [a for p in pairs for a in p]
    return pl.pallas_call(
        functools.partial(unpack_body, half_n, len(pairs)),
        out_shape=(shape,) * 3,
        cost_estimate=pl.CostEstimate(flops=1_000_000_000, bytes_accessed=1 << 22, transcendentals=0),
        compiler_params=pltpu.CompilerParams(vmem_limit_bytes=VMEM_BIG),
        name="unpack",
    )(*flat)


def shard_index(z, y, first, a, b, sign):
    dz, dy = (a, b) if first == "z" else (b, a)
    return lax.rem(z + sign * dz + 4, 4) * 4 + lax.rem(y + sign * dy + 4, 4)


def experts_body(n_sets, last, first, has_prev, *refs):
    place = refs[0]
    r_refs = refs[1 : 1 + n_sets]
    c_refs = refs[1 + n_sets : 1 + 2 * n_sets]
    at = 1 + 2 * n_sets
    w_refs = refs[at : at + 5]
    at += 5 + (2 if has_prev else 0)
    o_ref, dr_ref = refs[at : at + 2]
    g_refs = refs[at + 2 : at + 7]
    wgu, wd, ab, dh, hid, dab, dwgu, dwd = refs[at + 7 :]
    z, y = place[0], place[1]
    stride, width = r_refs[0].shape[1:]
    rows = width // 16
    half = rows // 2
    packed = rows + half
    f_pad = wd.shape[1]
    low = lax.broadcasted_iota(jnp.int32, (half, LANES), 1) < LANES // 2

    for a in range(4):
        for b in range(4):
            if a == 2:
                ref, slot = (w_refs[3], b) if b < 2 else (w_refs[4], b - 2)
            else:
                ref, slot = w_refs[(0, 1, None, 2)[a]], b
            k = shard_index(z, y, last, a, b, -1)
            row0 = pl.multiple_of(k * rows, rows)
            for m in range(3):
                base = m * packed
                dst, col = (wgu, m * f_pad) if m < 2 else (wd, 0)
                dst[pl.ds(row0, rows), col : col + LANES] = ref[slot, 0, base : base + rows, :]
                rest = ref[slot, 0, base + rows : base + packed, :].astype(jnp.float32)
                top = jnp.where(low, rest, 0.0)
                bottom = jnp.where(low, pltpu.roll(rest, LANES // 2, 1), 0.0)
                dst[pl.ds(row0, rows), col + LANES : col + 2 * LANES] = jnp.concatenate([top, bottom], axis=0).astype(dst.dtype)

    rows_all = jnp.concatenate([r[0] for r in r_refs], axis=0)
    cots_all = jnp.concatenate([c[0] for c in c_refs], axis=0)
    ab[...] = jnp.dot(rows_all, wgu[...], preferred_element_type=jnp.float32)
    dh[...] = jnp.dot(cots_all, wd[...], preferred_element_type=jnp.float32)

    def act(q, carry):
        r0 = pl.multiple_of(q * 32, 32)
        pre = ab[pl.ds(r0, 32), :f_pad]
        up = ab[pl.ds(r0, 32), f_pad:]
        grad = dh[pl.ds(r0, 32), :]
        sig = jax.nn.sigmoid(pre)
        silu = pre * sig
        hid[pl.ds(r0, 32), :] = (silu * up).astype(jnp.bfloat16)
        dab[pl.ds(r0, 32), :f_pad] = (grad * up * sig * (1.0 + pre * (1.0 - sig))).astype(jnp.bfloat16)
        dab[pl.ds(r0, 32), f_pad:] = (grad * silu).astype(jnp.bfloat16)
        return carry

    lax.fori_loop(0, n_sets * stride // 32, act, 0)

    nt = (((1,), (1,)), ((), ()))
    tn = (((0,), (0,)), ((), ()))
    out = lax.dot_general(hid[...], wd[...], nt, preferred_element_type=jnp.float32).astype(jnp.bfloat16)
    for s in range(n_sets):
        o_ref[s, 0] = out[s * stride : (s + 1) * stride]
    back = lax.dot_general(dab[...], wgu[...], nt, preferred_element_type=jnp.float32).astype(jnp.bfloat16)
    for s in range(n_sets):
        dr_ref[s, 0] = back[s * stride : (s + 1) * stride]
    dwgu[...] = lax.dot_general(rows_all, dab[...], tn, preferred_element_type=jnp.float32)
    dwd[...] = lax.dot_general(cots_all, hid[...], tn, preferred_element_type=jnp.float32)

    for a in range(4):
        for b in range(4):
            if a == 2:
                ref, slot = (g_refs[3], b) if b < 2 else (g_refs[4], b - 2)
            else:
                ref, slot = g_refs[(0, 1, None, 2)[a]], b
            k = shard_index(z, y, first, a, b, 1)
            row0 = pl.multiple_of(k * rows, rows)
            for m in range(3):
                base = m * packed
                src, col = (dwgu, m * f_pad) if m < 2 else (dwd, 0)
                ref[slot, 0, base : base + rows, :] = src[pl.ds(row0, rows), col : col + LANES]
                rest = src[pl.ds(row0, rows), col + LANES : col + 2 * LANES]
                ref[slot, 0, base + rows : base + packed, :] = jnp.where(low, rest[:half], pltpu.roll(rest[half:], LANES // 2, 1))


def experts(place, r_sets, c_sets, w_arrays, prev, colour, start, count, n_loc):
    n_sets = len(r_sets)
    n_mine, stride, width = r_sets[0].shape
    half_n = n_loc // 2
    packed = w_arrays[0].shape[2]
    off = colour * half_n + start
    first, last = ("y", "z") if colour == 0 else ("z", "y")
    total = 2 * count

    def mine(i):
        return jnp.where(i < count, off + i, n_loc + off + i - count)

    def held(i):
        return jnp.where(i < count, start + i, half_n + start + i - count)

    tok_spec = pl.BlockSpec((1, stride, width), lambda i: (mine(i), 0, 0))
    out_spec = pl.BlockSpec((n_sets, 1, stride, width), lambda i: (0, mine(i), 0, 0))
    out_shape = jax.ShapeDtypeStruct((n_sets, n_mine, stride, width), jnp.bfloat16)
    f_pad = 2 * LANES
    m_rows = n_sets * stride
    w_specs = [pl.BlockSpec((w.shape[0], 1, packed, LANES), lambda i: (0, held(i), 0, 0)) for w in w_arrays]
    g_slots = (4, 4, 4, 2, 2)
    g_specs = [pl.BlockSpec((n, 1, packed, LANES), lambda i: (0, i, 0, 0)) for n in g_slots]
    g_shapes = [jax.ShapeDtypeStruct((n, total, packed, LANES), jnp.float32) for n in g_slots]
    in_specs = [pl.BlockSpec(memory_space=pltpu.SMEM)] + [tok_spec] * (2 * n_sets) + w_specs
    args = [place, *r_sets, *c_sets, *w_arrays]
    aliases = {}
    if prev is not None:
        aliases = {len(args): 0, len(args) + 1: 1}
        in_specs += [pl.BlockSpec(memory_space=pl.ANY)] * 2
        args += list(prev)
    res = pl.pallas_call(
        functools.partial(experts_body, n_sets, last, first, prev is not None),
        grid=(total,),
        out_shape=[out_shape, out_shape] + g_shapes,
        in_specs=in_specs,
        out_specs=[out_spec, out_spec] + g_specs,
        scratch_shapes=[
            pltpu.VMEM((width, 2 * f_pad), jnp.bfloat16),
            pltpu.VMEM((width, f_pad), jnp.bfloat16),
            pltpu.VMEM((m_rows, 2 * f_pad), jnp.float32),
            pltpu.VMEM((m_rows, f_pad), jnp.float32),
            pltpu.VMEM((m_rows, f_pad), jnp.bfloat16),
            pltpu.VMEM((m_rows, 2 * f_pad), jnp.bfloat16),
            pltpu.VMEM((width, 2 * f_pad), jnp.float32),
            pltpu.VMEM((width, f_pad), jnp.float32),
        ],
        input_output_aliases=aliases,
        compiler_params=pltpu.CompilerParams(dimension_semantics=("arbitrary",), vmem_limit_bytes=VMEM_BIG),
        cost_estimate=pl.CostEstimate(flops=3_000_000_000 * total, bytes_accessed=6_000_000 * total, transcendentals=0),
        name="experts",
    )(*args)
    return (res[0], res[1]), res[2:]


def solution(mesh):
    n_pos = mesh.shape["expert"]
    chips_x = n_pos // 2
    row_spec = P(("rep", "expert", "data"), None)
    wide_spec = P("expert", "data", None)
    down_spec = P("expert", None, "data")
    wide_out = P(("rep", "expert"), "data", None)
    down_out = P(("rep", "expert"), None, "data")

    def y_perm(d):
        return [(z * 4 + y, z * 4 + (y + d) % 4) for z in range(4) for y in range(4)]

    def z_perm(d):
        return [(z * 4 + y, (z + d) % 4 * 4 + y) for z in range(4) for y in range(4)]

    perms = {"y": y_perm, "z": z_perm}
    partner = [(p, (p + n_pos // 2) % n_pos) for p in range(n_pos)]
    mate = [(p, p ^ 1) for p in range(n_pos)]
    to_neighbour = [(p, (p + (2 if p % 2 == 0 else -2)) % n_pos) for p in range(n_pos)]
    to_home = [(b, a) for a, b in to_neighbour]

    def step_along(v, axis, d):
        return lax.ppermute(v, "data", perms[axis](d))

    def gather_ring(v, axis, cut):
        one = step_along(v, axis, 1)
        three = step_along(v, axis, 3)
        two_a = step_along(one[:cut], axis, 1)
        two_b = step_along(three[cut:], axis, 3)
        return v, one, three, two_a, two_b

    def scatter_ring(parts, axis, cut):
        zero, one, three, two_a, two_b = parts
        in_a = step_along(two_a, axis, 1)
        in_b = step_along(two_b, axis, 3)
        one = one.at[:cut].add(in_a)
        three = three.at[cut:].add(in_b)
        return zero, step_along(one, axis, 1), step_along(three, axis, 3)

    def local_step(tok_in, expert_idx, gate_wt, w_gate, w_up, w_down, grad_out):
        tokens, top_k = expert_idx.shape
        width = tok_in.shape[1]
        n_loc, rows, f_dim = w_gate.shape
        n_exp = n_loc * n_pos
        cap = (5 * top_k * tokens + 4 * n_exp - 1) // (4 * n_exp)
        stride = ceil_to(cap, 16)
        half_n = n_loc // 2
        data_id = lax.axis_index("data")
        pos_id = lax.axis_index("expert")
        place = jnp.stack([data_id // 4, data_id % 4]).astype(jnp.int32)
        groups = jnp.stack([pos_id, (pos_id + n_pos // 2) % n_pos]).astype(jnp.int32)

        own = pack_weights(w_gate, w_up, jnp.swapaxes(w_down, 1, 2))
        other = lax.ppermute(own, "expert", partner)
        held = []
        for colour, (first, last) in enumerate((("y", "z"), ("z", "y"))):
            part = slice(colour * half_n, (colour + 1) * half_n)
            v = jnp.concatenate([own[part], other[part]], axis=0)
            v, one, three, two_a, two_b = gather_ring(v, first, half_n)
            four = jnp.stack([v, one, jnp.concatenate([two_a, two_b], axis=0), three])
            held.append(gather_ring(four, last, 2))

        lists, gates = make_lists(expert_idx, gate_wt)
        sets = [(tok_in, grad_out, gates, lists)]
        sets.append(tuple(lax.ppermute(a, "expert", mate) for a in sets[0]))
        sets.append(tuple(lax.ppermute(a, "expert", to_neighbour) for a in sets[0]))
        sets.append(tuple(lax.ppermute(a, "expert", mate) for a in sets[2]))
        sent = [dispatch(groups, li, g, x, d, stride, cap, n_loc) for x, d, g, li in sets]
        r_sets, c_sets = [s[0] for s in sent], [s[1] for s in sent]

        prev = None
        grads = {}
        n_chunks = 2
        count = half_n // n_chunks
        for chunk in range(n_chunks):
            for colour in range(2):
                prev, parts = experts(place, r_sets, c_sets, held[colour], prev, colour, chunk * count, count, n_loc)
                first, last = ("y", "z") if colour == 0 else ("z", "y")
                zero, one, three = scatter_ring((parts[0], parts[1], parts[2], parts[3], parts[4]), first, 2)
                s = [zero[q] + one[q] + three[q] for q in range(4)]
                zero, one, three = scatter_ring((s[0], s[1], s[3], s[2][:count], s[2][count:]), last, count)
                mine = zero[:count] + one[:count] + three[:count]
                theirs = zero[count:] + one[count:] + three[count:]
                grads[colour, chunk] = (mine, lax.ppermute(theirs, "expert", partner))
        o_all, dr_all = prev

        sums = [combine(k, groups, sets[k][3], sets[k][2], o_all, dr_all, tokens, cap, n_loc) for k in (3, 2, 1, 0)][::-1]
        near = sums[2] + lax.ppermute(sums[3], "expert", mate)
        far = lax.ppermute(near, "expert", to_home)
        total = sums[0] + lax.ppermute(sums[1], "expert", mate) + far
        tok_out = (tok_in.astype(jnp.float32) + total[:, :width]).astype(jnp.bfloat16)
        grad_in = (grad_out.astype(jnp.float32) + total[:, width:]).astype(jnp.bfloat16)

        order = [grads[colour, chunk] for colour in range(2) for chunk in range(n_chunks)]
        gg, gu, gd = unpack_grads(order, n_loc, rows, f_dim)
        return tok_out, grad_in, gg, gu, jnp.swapaxes(gd, 1, 2)

    return jax.shard_map(local_step, mesh=mesh, in_specs=(row_spec, row_spec, row_spec, wide_spec, wide_spec, down_spec, row_spec), out_specs=(row_spec, row_spec, wide_out, wide_out, down_out), check_vma=False)
```
